8 devices in a mesh: dp: 1 (over z), sp: 8 (over y, x, core).
Axes of the slice: x: 2, y: 2, z: 1, core: 2. Of those that a mesh axis runs over, the one named last changes fastest.
Arguments:
- x_in: bfloat16 [4, 2048, 4608], P('dp', 'sp')
- dy_in: bfloat16 [4, 2048, 4608], P('dp', 'sp')
- positions: int32 [2048], P(('dp', 'sp'))
- w_q: bfloat16 [4608, 4096], replicated
- w_k: bfloat16 [4608, 2048], replicated
- w_v: bfloat16 [4608, 2048], replicated
- w_o: bfloat16 [4096, 4608], replicated
- w_pre: float32 [4608], replicated
- w_post: float32 [4608], replicated
- q_norm: float32 [128], replicated
- k_norm: float32 [128], replicated
Outputs:
- output 1: bfloat16 [4, 2048, 4608], P('dp', 'sp')
- output 2: bfloat16 [4, 2048, 4608], P('dp', 'sp')
- output 3: bfloat16 [4608, 4096], P('dp')
- output 4: bfloat16 [4608, 2048], P('dp')
- output 5: bfloat16 [4608, 2048], P('dp')
- output 6: bfloat16 [4096, 4608], P('dp')
- output 7: float32 [4608], P('dp')
- output 8: float32 [4608], P('dp')
- output 9: float32 [128], P('dp')
- output 10: float32 [128], P('dp')
All inputs are finite; a program needn't handle non-finite values.
Results may differ from the reference program's by a relative error of at most 0.02.
Values are sent between devices in bfloat16 or wider.
A program may use at most 1 GiB of HBM per device.

```python
import functools
import jax
import jax.numpy as jnp
from jax import lax

B = 4
SEQ = 2048
D = 4608
H = 32
K = 16
HEAD = 128

EPS = 1e-6
ROPE_BASE = 1000000.0
ROPE_SCALE = 8.0
NEG_BIG = -1e30
Q_ROWS = min(128, SEQ)


def setup_inputs(seed: int = 0, part: int = 0) -> dict:
    base_key = jax.random.key(seed)
    own = jax.random.split(jax.random.fold_in(base_key, part), 4)
    shared = jax.random.split(base_key, 8)
    x_in = jax.random.normal(own[0], (B, SEQ, D), jnp.float32).astype(jnp.bfloat16)
    dy_in = jax.random.normal(own[1], (B, SEQ, D), jnp.float32).astype(jnp.bfloat16)
    start = jax.random.randint(own[2], (1,), 0, 1000)
    gaps = jax.random.randint(own[3], (SEQ,), 1, 5)
    positions = (start + jnp.cumsum(gaps) - gaps[0]).astype(jnp.int32)
    w_q = (jax.random.normal(shared[0], (D, H * HEAD), jnp.float32) * D ** -0.5).astype(jnp.bfloat16)
    w_k = (jax.random.normal(shared[1], (D, K * HEAD), jnp.float32) * D ** -0.5).astype(jnp.bfloat16)
    w_v = (jax.random.normal(shared[2], (D, K * HEAD), jnp.float32) * D ** -0.5).astype(jnp.bfloat16)
    w_o = (jax.random.normal(shared[3], (H * HEAD, D), jnp.float32) * (H * HEAD) ** -0.5).astype(jnp.bfloat16)
    w_pre = 0.3 * jax.random.normal(shared[4], (D,), jnp.float32)
    w_post = 0.3 * jax.random.normal(shared[5], (D,), jnp.float32)
    q_norm = 0.3 + 0.3 * jax.random.normal(shared[6], (HEAD,), jnp.float32)
    k_norm = 0.3 + 0.3 * jax.random.normal(shared[7], (HEAD,), jnp.float32)
    return {'x_in': x_in, 'dy_in': dy_in, 'positions': positions, 'w_q': w_q, 'w_k': w_k, 'w_v': w_v, 'w_o': w_o, 'w_pre': w_pre, 'w_post': w_post, 'q_norm': q_norm, 'k_norm': k_norm}


def rms_scale(x_f32, weight):
    inv_rms = lax.rsqrt(jnp.mean(x_f32 * x_f32, axis=-1, keepdims=True) + EPS)
    return x_f32 * inv_rms * (1.0 + weight)


def norm_rope(heads_f32, weight, cosines, sines):
    half_dim = HEAD // 2
    normed = rms_scale(heads_f32, weight)
    first = normed[..., :half_dim]
    second = normed[..., half_dim:]
    cos_b = cosines[None, :, None, :]
    sin_b = sines[None, :, None, :]
    return jnp.concatenate([first * cos_b - second * sin_b, second * cos_b + first * sin_b], axis=-1)


def attention(q_rot, k_rot, v_heads):
    group = H // K
    blocks = SEQ // Q_ROWS
    q_blocks = jnp.moveaxis(q_rot.reshape(B, blocks, Q_ROWS, K, group, HEAD), 1, 0)
    key_f32 = k_rot.astype(jnp.float32)
    val_f32 = v_heads.astype(jnp.float32)
    col_ids = jnp.arange(SEQ)

    def one_block(item):
        q_blk, index = item
        scores = jnp.einsum('bqkgh,bskh->bkgqs', q_blk.astype(jnp.float32), key_f32) * HEAD ** -0.5
        row_ids = index * Q_ROWS + jnp.arange(Q_ROWS)
        scores = jnp.where(row_ids[:, None] >= col_ids[None, :], scores, NEG_BIG)
        attn_prob = jax.nn.softmax(scores, axis=-1).astype(jnp.bfloat16).astype(jnp.float32)
        return jnp.einsum('bkgqs,bskh->bqkgh', attn_prob, val_f32).astype(jnp.bfloat16)

    block_out = lax.map(jax.checkpoint(one_block), (q_blocks, jnp.arange(blocks)))
    return jnp.moveaxis(block_out, 0, 1).reshape(B, SEQ, H, HEAD)


def forward(positions, x_in, w_q, w_k, w_v, w_o, w_pre, w_post, q_norm, k_norm):
    x_f32 = x_in.astype(jnp.float32)
    normed = rms_scale(x_f32, w_pre).astype(jnp.bfloat16).astype(jnp.float32)
    q_proj = jnp.einsum('bsd,dn->bsn', normed, w_q.astype(jnp.float32)).astype(jnp.bfloat16)
    k_proj = jnp.einsum('bsd,dn->bsn', normed, w_k.astype(jnp.float32)).astype(jnp.bfloat16)
    v_proj = jnp.einsum('bsd,dn->bsn', normed, w_v.astype(jnp.float32)).astype(jnp.bfloat16)
    half_dim = HEAD // 2
    inv_freq = ROPE_BASE ** (-jnp.arange(half_dim, dtype=jnp.float32) * 2.0 / HEAD)
    angles = (positions.astype(jnp.float32) / ROPE_SCALE)[:, None] * inv_freq[None, :]
    cosines = jnp.cos(angles)
    sines = jnp.sin(angles)
    q_rot = norm_rope(q_proj.reshape(B, SEQ, H, HEAD).astype(jnp.float32), q_norm, cosines, sines).astype(jnp.bfloat16)
    k_rot = norm_rope(k_proj.reshape(B, SEQ, K, HEAD).astype(jnp.float32), k_norm, cosines, sines).astype(jnp.bfloat16)
    v_heads = v_proj.reshape(B, SEQ, K, HEAD)
    attn_out = attention(q_rot, k_rot, v_heads)
    proj = jnp.einsum('bsn,nd->bsd', attn_out.reshape(B, SEQ, H * HEAD).astype(jnp.float32), w_o.astype(jnp.float32)).astype(jnp.bfloat16)
    return (x_f32 + rms_scale(proj.astype(jnp.float32), w_post)).astype(jnp.bfloat16)


def reference(x_in, dy_in, positions, w_q, w_k, w_v, w_o, w_pre, w_post, q_norm, k_norm):
    y_out, pullback = jax.vjp(functools.partial(forward, positions), x_in, w_q, w_k, w_v, w_o, w_pre, w_post, q_norm, k_norm)
    grads = pullback(dy_in)
    return (y_out, grads[0], grads[1], grads[2], grads[3], grads[4], grads[5], grads[6], grads[7], grads[8])
```

```python
import functools
import jax
import jax.numpy as jnp
from jax import lax
from jax.experimental import pallas as pl
from jax.experimental.pallas import tpu as pltpu
from jax.sharding import PartitionSpec as P

EPS = 1e-6
ROPE_BASE = 1000000.0
ROPE_SCALE = 8.0
NEG_BIG = -1e30
LOG2E = 1.4426950408889634
ROWS = 256
CHUNKS = (2, 2)


def rms_scale(x_f32, weight):
    inv_rms = lax.rsqrt(jnp.mean(x_f32 * x_f32, axis=-1, keepdims=True) + EPS)
    return x_f32 * inv_rms * (1.0 + weight)


def pre_norm(x_f32, weight):
    return rms_scale(x_f32, weight).astype(jnp.bfloat16)


def post_norm(proj, weight):
    return rms_scale(proj.astype(jnp.float32), weight)


def rope_tables(positions, head):
    half_dim = head // 2
    inv_freq = ROPE_BASE ** (-jnp.arange(half_dim, dtype=jnp.float32) * 2.0 / head)
    angles = (positions.astype(jnp.float32) / ROPE_SCALE)[:, None] * inv_freq[None, :]
    cosines = jnp.cos(angles)
    sines = jnp.sin(angles)
    return jnp.concatenate([cosines, cosines], axis=-1), jnp.concatenate([-sines, sines], axis=-1)


def dot_nt(a, b):
    return lax.dot_general(a, b, (((1,), (1,)), ((), ())), preferred_element_type=jnp.float32)


def dot_tn(a, b):
    return lax.dot_general(a, b, (((0,), (0,)), ((), ())), preferred_element_type=jnp.float32)


def dot_nn(a, b):
    return lax.dot_general(a, b, (((1,), (0,)), ((), ())), preferred_element_type=jnp.float32)


def rotate(x_bf, weight, cos_t, sin_t):
    normed = rms_scale(x_bf.astype(jnp.float32), weight)
    return (normed * cos_t + pltpu.roll(normed, normed.shape[-1] // 2, 1) * sin_t).astype(jnp.bfloat16)


def rotate_bwd(d_rot, x_bf, weight, cos_t, sin_t):
    d_f32 = d_rot.astype(jnp.float32)
    d_norm = d_f32 * cos_t - pltpu.roll(d_f32, d_f32.shape[-1] // 2, 1) * sin_t
    x = x_bf.astype(jnp.float32)
    inv_rms = lax.rsqrt(jnp.mean(x * x, axis=-1, keepdims=True) + EPS)
    unit = x * inv_rms
    scaled = d_norm * (1.0 + weight)
    dx = (scaled - unit * jnp.mean(scaled * unit, axis=-1, keepdims=True)) * inv_rms
    d_weight = jnp.sum((d_norm * unit).reshape(-1, 8, x.shape[-1]), axis=0)
    return dx.astype(jnp.bfloat16), d_weight


def causal(scores, fill):
    row_ids = lax.broadcasted_iota(jnp.int32, scores.shape, 0)
    col_ids = lax.broadcasted_iota(jnp.int32, scores.shape, 1)
    return jnp.where(row_ids >= col_ids, scores, fill)


def fwd_kernel(group, q_ref, k_ref, v_ref, cos_ref, sin_ref, wq_ref, wk_ref, o_ref, lse_ref, k_rot):
    seq, head = k_rot.shape
    member = lax.rem(pl.program_id(1), group)
    coef = head ** -0.5 * LOG2E
    wq = wq_ref[...]

    @pl.when(member == 0)
    def _():
        for start in range(0, seq, ROWS):
            rows = slice(start, start + ROWS)
            k_rot[rows, :] = rotate(k_ref[0, rows, :], wk_ref[...], cos_ref[rows, :], sin_ref[rows, :])

    for start in range(0, seq, ROWS):
        rows = slice(start, start + ROWS)
        q_rot = rotate(q_ref[0, rows, :], wq, cos_ref[rows, :], sin_ref[rows, :])
        s_diag = causal(dot_nt(q_rot, k_rot[rows, :]), NEG_BIG)
        row_max = jnp.max(s_diag, axis=-1, keepdims=True)
        if start:
            s_off = dot_nt(q_rot, k_rot[:start, :])
            row_max = jnp.maximum(row_max, jnp.max(s_off, axis=-1, keepdims=True))
        e_diag = jnp.exp2((s_diag - row_max) * coef)
        row_sum = jnp.sum(e_diag, axis=-1, keepdims=True)
        if start:
            e_off = jnp.exp2((s_off - row_max) * coef)
            row_sum = row_sum + jnp.sum(e_off, axis=-1, keepdims=True)
        inv_sum = 1.0 / row_sum
        out = dot_nn((e_diag * inv_sum).astype(jnp.bfloat16), v_ref[0, rows, :])
        if start:
            out = out + dot_nn((e_off * inv_sum).astype(jnp.bfloat16), v_ref[0, :start, :])
        o_ref[0, rows, :] = out.astype(jnp.bfloat16)
        lse = jnp.broadcast_to(row_max * coef + jnp.log2(row_sum), (ROWS, head))
        lanes = lax.broadcasted_iota(jnp.int32, (ROWS, head), 1)
        owner = lax.div(lanes, head // group)
        lse_ref[0, 0, rows, :] = jnp.where(owner >= member, lse, lse_ref[0, 0, rows, :])


def bwd_kernel(group, q_ref, k_ref, v_ref, do_ref, lse_ref, cos_ref, sin_ref, wq_ref, wk_ref,
               dq_ref, dk_ref, dv_ref, dwq_ref, dwk_ref, k_rot, dk_acc, dv_acc):
    seq, head = k_rot.shape
    member = lax.rem(pl.program_id(1), group)
    scale = head ** -0.5
    coef = scale * LOG2E
    wq = wq_ref[...]
    wk = wk_ref[...]

    @pl.when(jnp.logical_and(pl.program_id(0) == 0, pl.program_id(1) == 0))
    def _():
        dwq_ref[...] = jnp.zeros_like(dwq_ref)
        dwk_ref[...] = jnp.zeros_like(dwk_ref)

    @pl.when(member == 0)
    def _():
        dk_acc[...] = jnp.zeros_like(dk_acc)
        dv_acc[...] = jnp.zeros_like(dv_acc)
        for start in range(0, seq, ROWS):
            rows = slice(start, start + ROWS)
            k_rot[rows, :] = rotate(k_ref[0, rows, :], wk, cos_ref[rows, :], sin_ref[rows, :])

    for start in range(0, seq, ROWS):
        rows = slice(start, start + ROWS)
        q_raw = q_ref[0, rows, :]
        q_rot = rotate(q_raw, wq, cos_ref[rows, :], sin_ref[rows, :])
        d_out = do_ref[0, rows, :]
        lse_all = lse_ref[0, 0, rows, :]
        lse = lse_all[:, :1]
        for other in range(1, group):
            at = other * (head // group)
            lse = jnp.where(member == other, lse_all[:, at:at + 1], lse)
        p_diag = causal(jnp.exp2(dot_nt(q_rot, k_rot[rows, :]) * coef - lse), 0.0)
        dp_diag = dot_nt(d_out, v_ref[0, rows, :])
        delta = jnp.sum(p_diag * dp_diag, axis=-1, keepdims=True)
        if start:
            p_off = jnp.exp2(dot_nt(q_rot, k_rot[:start, :]) * coef - lse)
            dp_off = dot_nt(d_out, v_ref[0, :start, :])
            delta = delta + jnp.sum(p_off * dp_off, axis=-1, keepdims=True)
        ds_diag = (p_diag * (dp_diag - delta) * scale).astype(jnp.bfloat16)
        dq = dot_nn(ds_diag, k_rot[rows, :])
        dk_acc[rows, :] += dot_tn(ds_diag, q_rot)
        dv_acc[rows, :] += dot_tn(p_diag.astype(jnp.bfloat16), d_out)
        if start:
            ds_off = (p_off * (dp_off - delta) * scale).astype(jnp.bfloat16)
            dq = dq + dot_nn(ds_off, k_rot[:start, :])
            dk_acc[:start, :] += dot_tn(ds_off, q_rot)
            dv_acc[:start, :] += dot_tn(p_off.astype(jnp.bfloat16), d_out)
        dq_ref[0, rows, :], dw = rotate_bwd(dq.astype(jnp.bfloat16), q_raw, wq, cos_ref[rows, :], sin_ref[rows, :])
        dwq_ref[...] += dw

    @pl.when(member == group - 1)
    def _():
        for start in range(0, seq, ROWS):
            rows = slice(start, start + ROWS)
            dk_ref[0, rows, :], dw = rotate_bwd(dk_acc[rows, :].astype(jnp.bfloat16), k_ref[0, rows, :], wk, cos_ref[rows, :], sin_ref[rows, :])
            dwk_ref[...] += dw
            dv_ref[0, rows, :] = dv_acc[rows, :].astype(jnp.bfloat16)


def attention_specs(seq, head, heads, group):
    kv = heads // group
    q_spec = pl.BlockSpec((1, seq, head), lambda b, h: (b, 0, h))
    k_spec = pl.BlockSpec((1, seq, head), lambda b, h: (b, 0, heads + h // group))
    v_spec = pl.BlockSpec((1, seq, head), lambda b, h: (b, 0, heads + kv + h // group))
    kv_spec = pl.BlockSpec((1, seq, head), lambda b, h: (b, 0, h // group))
    lse_spec = pl.BlockSpec((1, 1, seq, head), lambda b, h: (b, h // group, 0, 0))
    tab_spec = pl.BlockSpec((seq, head), lambda b, h: (0, 0))
    w_spec = pl.BlockSpec((1, head), lambda b, h: (0, 0))
    dw_spec = pl.BlockSpec((8, head), lambda b, h: (0, 0))
    return q_spec, k_spec, v_spec, kv_spec, lse_spec, tab_spec, w_spec, dw_spec


def attention_fwd(qkv, cos_t, sin_t, wq, wk, heads, group):
    batch, seq, _ = qkv.shape
    head = cos_t.shape[1]
    q_spec, k_spec, v_spec, _, lse_spec, tab_spec, w_spec, _ = attention_specs(seq, head, heads, group)
    flops = batch * heads * seq * seq * head * 2
    return pl.pallas_call(
        functools.partial(fwd_kernel, group),
        grid=(batch, heads),
        in_specs=[q_spec, k_spec, v_spec, tab_spec, tab_spec, w_spec, w_spec],
        out_specs=[q_spec, lse_spec],
        out_shape=[jax.ShapeDtypeStruct((batch, seq, heads * head), jnp.bfloat16),
                   jax.ShapeDtypeStruct((batch, heads // group, seq, head), jnp.float32)],
        scratch_shapes=[pltpu.VMEM((seq, head), jnp.bfloat16)],
        compiler_params=pltpu.CompilerParams(dimension_semantics=('arbitrary', 'arbitrary'), vmem_limit_bytes=56 * 2 ** 20),
        cost_estimate=pl.CostEstimate(flops=flops, bytes_accessed=batch * seq * 3000, transcendentals=batch * heads * seq * seq // 2),
        name='attention_fwd',
    )(qkv, qkv, qkv, cos_t, sin_t, wq, wk)


def attention_bwd(qkv, d_out, lse, cos_t, sin_t, wq, wk, heads, group):
    batch, seq, _ = qkv.shape
    head = cos_t.shape[1]
    kv = heads // group
    q_spec, k_spec, v_spec, kv_spec, lse_spec, tab_spec, w_spec, dw_spec = attention_specs(seq, head, heads, group)
    flops = batch * heads * seq * seq * head * 5
    return pl.pallas_call(
        functools.partial(bwd_kernel, group),
        grid=(batch, heads),
        in_specs=[q_spec, k_spec, v_spec, q_spec, lse_spec, tab_spec, tab_spec, w_spec, w_spec],
        out_specs=[q_spec, kv_spec, kv_spec, dw_spec, dw_spec],
        out_shape=[jax.ShapeDtypeStruct((batch, seq, heads * head), jnp.bfloat16),
                   jax.ShapeDtypeStruct((batch, seq, kv * head), jnp.bfloat16),
                   jax.ShapeDtypeStruct((batch, seq, kv * head), jnp.bfloat16),
                   jax.ShapeDtypeStruct((8, head), jnp.float32),
                   jax.ShapeDtypeStruct((8, head), jnp.float32)],
        scratch_shapes=[pltpu.VMEM((seq, head), jnp.bfloat16), pltpu.VMEM((seq, head), jnp.float32), pltpu.VMEM((seq, head), jnp.float32)],
        compiler_params=pltpu.CompilerParams(dimension_semantics=('arbitrary', 'arbitrary'), vmem_limit_bytes=56 * 2 ** 20),
        cost_estimate=pl.CostEstimate(flops=flops, bytes_accessed=batch * seq * 6000, transcendentals=batch * heads * seq * seq // 2),
        name='attention_bwd',
    )(qkv, qkv, qkv, d_out, lse, cos_t, sin_t, wq, wk)


def ein(spec, a, b):
    return jnp.einsum(spec, a, b, preferred_element_type=jnp.float32)


def solution(mesh):
    n_dev = mesh.shape['sp']

    def to_tokens(arr):
        return lax.all_to_all(arr, 'sp', 1, 2, tiled=True)

    def gather_tokens(arr):
        return lax.all_gather(arr, 'sp', axis=1, tiled=True)

    def device_step(x_in, dy_in, positions, w_q, w_k, w_v, w_o, w_pre, w_post, q_norm, k_norm):
        head = q_norm.shape[0]
        q_cols = w_q.shape[1] // n_dev
        kv_cols = w_k.shape[1] // n_dev
        heads = q_cols // head
        group = q_cols // kv_cols
        me = lax.axis_index('sp')
        bounds = []
        at = 0
        for size in CHUNKS:
            bounds.append((at, at + size))
            at += size
        parts = range(len(bounds))

        x_f32 = [x_in[lo:hi].astype(jnp.float32) for lo, hi in bounds]
        pre = [jax.vjp(pre_norm, x, w_pre) for x in x_f32]
        normed = [gather_tokens(p[0]) for p in pre]
        cos_t, sin_t = rope_tables(lax.all_gather(positions, 'sp', axis=0, tiled=True), head)
        w_loc = jnp.concatenate([lax.dynamic_slice_in_dim(w_q, me * q_cols, q_cols, 1),
                                 lax.dynamic_slice_in_dim(w_k, me * kv_cols, kv_cols, 1),
                                 lax.dynamic_slice_in_dim(w_v, me * kv_cols, kv_cols, 1)], axis=1)
        wo_loc = lax.dynamic_slice_in_dim(w_o, me * q_cols, q_cols, 0)
        wq_row = q_norm[None, :]
        wk_row = k_norm[None, :]

        qkv, o_loc, lse, y_parts, d_proj, d_proj_all = [], [], [], [], [], []
        dw_post = 0.0
        for c in parts:
            lo, hi = bounds[c]
            qkv.append(ein('bsd,dn->bsn', normed[c], w_loc).astype(jnp.bfloat16))
            o_c, lse_c = attention_fwd(qkv[c], cos_t, sin_t, wq_row, wk_row, heads, group)
            o_loc.append(o_c)
            lse.append(lse_c)
            proj = ein('bsn,nd->bsd', to_tokens(o_c), w_o).astype(jnp.bfloat16)
            post, post_pull = jax.vjp(post_norm, proj, w_post)
            y_parts.append((x_f32[c] + post).astype(jnp.bfloat16))
            d_c, dwp = post_pull(dy_in[lo:hi].astype(jnp.float32))
            dw_post = dw_post + dwp
            d_proj_all.append(gather_tokens(d_c))

        d_qkv, d_tok = [], []
        dq_norm = 0.0
        dk_norm = 0.0
        for c in parts:
            d_o = ein('bsd,nd->bsn', d_proj_all[c], wo_loc).astype(jnp.bfloat16)
            dq, dk, dv, dwq, dwk = attention_bwd(qkv[c], d_o, lse[c], cos_t, sin_t, wq_row, wk_row, heads, group)
            dq_norm = dq_norm + jnp.sum(dwq, axis=0)
            dk_norm = dk_norm + jnp.sum(dwk, axis=0)
            d_qkv.append((dq, dk, dv))
            d_tok.append((to_tokens(dq), to_tokens(dk), to_tokens(dv)))

        dw_o = sum(ein('bsn,bsd->nd', o_loc[c], d_proj_all[c]) for c in parts).astype(jnp.bfloat16)
        dw_o = lax.all_gather(dw_o, 'sp', axis=0, tiled=True)
        dw = []
        for j in range(3):
            local = sum(ein('bsd,bsn->dn', normed[c], d_qkv[c][j]) for c in parts).astype(jnp.bfloat16)
            dw.append(lax.all_gather(local, 'sp', axis=1, tiled=True))

        dx_parts = []
        dw_pre = 0.0
        for c in parts:
            lo, hi = bounds[c]
            dq, dk, dv = d_tok[c]
            d_normed = (ein('bsn,dn->bsd', dq, w_q) + ein('bsn,dn->bsd', dk, w_k) + ein('bsn,dn->bsd', dv, w_v)).astype(jnp.bfloat16)
            dx_norm, dwp = pre[c][1](d_normed)
            dw_pre = dw_pre + dwp
            dx_parts.append((dy_in[lo:hi].astype(jnp.float32) + dx_norm).astype(jnp.bfloat16))

        sums = lax.psum((dw_pre, dw_post, dq_norm, dk_norm), 'sp')
        return (jnp.concatenate(y_parts, axis=0), jnp.concatenate(dx_parts, axis=0), dw[0], dw[1], dw[2], dw_o) + sums

    token_spec = P('dp', 'sp', None)
    return jax.shard_map(device_step, mesh=mesh,
                         in_specs=(token_spec, token_spec, P(('dp', 'sp')), P(None, None), P(None, None), P(None, None), P(None, None), P(None), P(None), P(None), P(None)),
                         out_specs=(token_spec, token_spec, P('dp', None), P('dp', None), P('dp', None), P('dp', None), P('dp'), P('dp'), P('dp'), P('dp')),
                         check_vma=False)
```

```python
import functools
import jax
import jax.numpy as jnp
from jax import lax
from jax.experimental import pallas as pl
from jax.experimental.pallas import tpu as pltpu
from jax.sharding import PartitionSpec as P

EPS = 1e-6
ROPE_BASE = 1000000.0
ROPE_SCALE = 8.0
NEG_BIG = -1e30
LOG2E = 1.4426950408889634
CHUNKS = (2, 1, 1)


def rms_scale(x_f32, weight):
    inv_rms = lax.rsqrt(jnp.mean(x_f32 * x_f32, axis=-1, keepdims=True) + EPS)
    return x_f32 * inv_rms * (1.0 + weight)


def pre_norm(x_f32, weight):
    return rms_scale(x_f32, weight).astype(jnp.bfloat16)


def post_norm(proj, weight):
    return rms_scale(proj.astype(jnp.float32), weight)


def rope_tables(positions, head):
    half_dim = head // 2
    inv_freq = ROPE_BASE ** (-jnp.arange(half_dim, dtype=jnp.float32) * 2.0 / head)
    angles = (positions.astype(jnp.float32) / ROPE_SCALE)[:, None] * inv_freq[None, :]
    cosines = jnp.cos(angles)
    sines = jnp.sin(angles)
    return jnp.concatenate([cosines, cosines], axis=-1), jnp.concatenate([-sines, sines], axis=-1)


def dot_nt(a, b):
    return lax.dot_general(a, b, (((1,), (1,)), ((), ())), preferred_element_type=jnp.float32)


def dot_tn(a, b):
    return lax.dot_general(a, b, (((0,), (0,)), ((), ())), preferred_element_type=jnp.float32)


def dot_nn(a, b):
    return lax.dot_general(a, b, (((1,), (0,)), ((), ())), preferred_element_type=jnp.float32)


def rotate(x_bf, weight, cos_t, sin_t):
    normed = rms_scale(x_bf.astype(jnp.float32), weight)
    return (normed * cos_t + pltpu.roll(normed, normed.shape[-1] // 2, 1) * sin_t).astype(jnp.bfloat16)


def rotate_bwd(d_rot, x_bf, weight, cos_t, sin_t):
    d_f32 = d_rot.astype(jnp.float32)
    d_norm = d_f32 * cos_t - pltpu.roll(d_f32, d_f32.shape[-1] // 2, 1) * sin_t
    x = x_bf.astype(jnp.float32)
    inv_rms = lax.rsqrt(jnp.mean(x * x, axis=-1, keepdims=True) + EPS)
    unit = x * inv_rms
    scaled = d_norm * (1.0 + weight)
    dx = (scaled - unit * jnp.mean(scaled * unit, axis=-1, keepdims=True)) * inv_rms
    d_weight = jnp.sum((d_norm * unit).reshape(-1, 8, x.shape[-1]), axis=0)
    return dx.astype(jnp.bfloat16), d_weight


def causal(scores, fill):
    row_ids = lax.broadcasted_iota(jnp.int32, scores.shape, 0)
    col_ids = lax.broadcasted_iota(jnp.int32, scores.shape, 1)
    return jnp.where(row_ids >= col_ids, scores, fill)


def prefix(ref, count):
    block = ref[:count, 0]
    return block.reshape(count * block.shape[1], block.shape[2])


def fwd_kernel(group, q_ref, k_ref, v_ref, cos_ref, sin_ref, wq_ref, wk_ref, o_ref, lse_ref, k_rot):
    n_blk, _, rows, head = q_ref.shape
    member = lax.rem(pl.program_id(1), group)
    coef = head ** -0.5 * LOG2E
    wq = wq_ref[...]

    @pl.when(member == 0)
    def _():
        for j in range(n_blk):
            k_rot[j, 0] = rotate(k_ref[j, 0], wk_ref[...], cos_ref[j], sin_ref[j])

    for j in range(n_blk):
        q_rot = rotate(q_ref[j, 0], wq, cos_ref[j], sin_ref[j])
        s_diag = causal(dot_nt(q_rot, k_rot[j, 0]), NEG_BIG)
        row_max = jnp.max(s_diag, axis=-1, keepdims=True)
        if j:
            s_off = dot_nt(q_rot, prefix(k_rot, j))
            row_max = jnp.maximum(row_max, jnp.max(s_off, axis=-1, keepdims=True))
        e_diag = jnp.exp2((s_diag - row_max) * coef)
        row_sum = jnp.sum(e_diag, axis=-1, keepdims=True)
        if j:
            e_off = jnp.exp2((s_off - row_max) * coef)
            row_sum = row_sum + jnp.sum(e_off, axis=-1, keepdims=True)
        inv_sum = 1.0 / row_sum
        out = dot_nn((e_diag * inv_sum).astype(jnp.bfloat16), v_ref[j, 0])
        if j:
            out = out + dot_nn((e_off * inv_sum).astype(jnp.bfloat16), prefix(v_ref, j))
        o_ref[j, 0] = out.astype(jnp.bfloat16)
        lse = jnp.broadcast_to(row_max * coef + jnp.log2(row_sum), (rows, head))
        lanes = lax.broadcasted_iota(jnp.int32, (rows, head), 1)
        owner = lax.div(lanes, head // group)
        lse_ref[0, 0, j] = jnp.where(owner >= member, lse, lse_ref[0, 0, j])


def bwd_kernel(group, heads, n_deps, q_ref, k_ref, v_ref, do_ref, lse_ref, cos_ref, sin_ref, wq_ref, wk_ref, *refs):
    d_ref, dwq_ref, dwk_ref, k_rot, dk_acc, dv_acc = refs[n_deps:]
    n_blk, _, rows, head = q_ref.shape
    member = lax.rem(pl.program_id(1), group)
    pair = lax.div(pl.program_id(1), group)
    q_lanes = pl.ds(pl.multiple_of(pl.program_id(1) * head, head), head)
    k_lanes = pl.ds(pl.multiple_of((heads + pair) * head, head), head)
    v_lanes = pl.ds(pl.multiple_of((heads + heads // group + pair) * head, head), head)
    scale = head ** -0.5
    coef = scale * LOG2E
    wq = wq_ref[...]
    wk = wk_ref[...]

    @pl.when(jnp.logical_and(pl.program_id(0) == 0, pl.program_id(1) == 0))
    def _():
        dwq_ref[...] = jnp.zeros_like(dwq_ref)
        dwk_ref[...] = jnp.zeros_like(dwk_ref)

    @pl.when(member == 0)
    def _():
        dk_acc[...] = jnp.zeros_like(dk_acc)
        dv_acc[...] = jnp.zeros_like(dv_acc)
        for j in range(n_blk):
            k_rot[j, 0] = rotate(k_ref[j, 0], wk, cos_ref[j], sin_ref[j])

    for j in range(n_blk):
        here = slice(j * rows, (j + 1) * rows)
        before = slice(0, j * rows)
        q_raw = q_ref[j, 0]
        q_rot = rotate(q_raw, wq, cos_ref[j], sin_ref[j])
        d_out = do_ref[j, 0]
        lse_all = lse_ref[0, 0, j]
        lse = lse_all[:, :1]
        for other in range(1, group):
            at = other * (head // group)
            lse = jnp.where(member == other, lse_all[:, at:at + 1], lse)
        p_diag = causal(jnp.exp2(dot_nt(q_rot, k_rot[j, 0]) * coef - lse), 0.0)
        dp_diag = dot_nt(d_out, v_ref[j, 0])
        delta = jnp.sum(p_diag * dp_diag, axis=-1, keepdims=True)
        if j:
            p_off = jnp.exp2(dot_nt(q_rot, prefix(k_rot, j)) * coef - lse)
            dp_off = dot_nt(d_out, prefix(v_ref, j))
            delta = delta + jnp.sum(p_off * dp_off, axis=-1, keepdims=True)
        ds_diag = (p_diag * (dp_diag - delta) * scale).astype(jnp.bfloat16)
        dq = dot_nn(ds_diag, k_rot[j, 0])
        dk_acc[here, :] += dot_tn(ds_diag, q_rot)
        dv_acc[here, :] += dot_tn(p_diag.astype(jnp.bfloat16), d_out)
        if j:
            ds_off = (p_off * (dp_off - delta) * scale).astype(jnp.bfloat16)
            dq = dq + dot_nn(ds_off, prefix(k_rot, j))
            dk_acc[before, :] += dot_tn(ds_off, q_rot)
            dv_acc[before, :] += dot_tn(p_off.astype(jnp.bfloat16), d_out)
        d_ref[j, 0, :, q_lanes], dw = rotate_bwd(dq.astype(jnp.bfloat16), q_raw, wq, cos_ref[j], sin_ref[j])
        dwq_ref[...] += dw

    @pl.when(member == group - 1)
    def _():
        for j in range(n_blk):
            here = slice(j * rows, (j + 1) * rows)
            d_ref[j, 0, :, k_lanes], dw = rotate_bwd(dk_acc[here, :].astype(jnp.bfloat16), k_ref[j, 0], wk, cos_ref[j], sin_ref[j])
            dwk_ref[...] += dw
            d_ref[j, 0, :, v_lanes] = dv_acc[here, :].astype(jnp.bfloat16)


def attention_specs(n_blk, rows, head, heads, group):
    kv = heads // group
    block = (n_blk, 1, rows, head)
    q_spec = pl.BlockSpec(block, lambda b, h: (0, b, 0, h))
    k_spec = pl.BlockSpec(block, lambda b, h: (0, b, 0, heads + h // group))
    v_spec = pl.BlockSpec(block, lambda b, h: (0, b, 0, heads + kv + h // group))
    lse_spec = pl.BlockSpec((1, 1, n_blk, rows, head), lambda b, h: (b, h // group, 0, 0, 0))
    tab_spec = pl.BlockSpec((n_blk, rows, head), lambda b, h: (0, 0, 0))
    w_spec = pl.BlockSpec((1, head), lambda b, h: (0, 0))
    dw_spec = pl.BlockSpec((8, head), lambda b, h: (0, 0))
    return q_spec, k_spec, v_spec, lse_spec, tab_spec, w_spec, dw_spec


def kernel_params():
    return pltpu.CompilerParams(dimension_semantics=('arbitrary', 'arbitrary'), vmem_limit_bytes=56 * 2 ** 20)


def attention_fwd(qkv, cos_t, sin_t, wq, wk, heads, group):
    n_blk, batch, rows, _ = qkv.shape
    head = cos_t.shape[2]
    pairs = batch * heads * (n_blk * rows) ** 2 // 2
    q_spec, k_spec, v_spec, lse_spec, tab_spec, w_spec, _ = attention_specs(n_blk, rows, head, heads, group)
    return pl.pallas_call(
        functools.partial(fwd_kernel, group),
        grid=(batch, heads),
        in_specs=[q_spec, k_spec, v_spec, tab_spec, tab_spec, w_spec, w_spec],
        out_specs=[q_spec, lse_spec],
        out_shape=[jax.ShapeDtypeStruct((n_blk, batch, rows, heads * head), jnp.bfloat16),
                   jax.ShapeDtypeStruct((batch, heads // group, n_blk, rows, head), jnp.float32)],
        scratch_shapes=[pltpu.VMEM((n_blk, 1, rows, head), jnp.bfloat16)],
        compiler_params=kernel_params(),
        cost_estimate=pl.CostEstimate(flops=pairs * head * 4, bytes_accessed=batch * n_blk * rows * 3000, transcendentals=pairs),
        name='attention_fwd',
    )(qkv, qkv, qkv, cos_t, sin_t, wq, wk)


def attention_bwd(qkv, d_out, lse, cos_t, sin_t, wq, wk, heads, group, deps=()):
    n_blk, batch, rows, cols = qkv.shape
    head = cos_t.shape[2]
    pairs = batch * heads * (n_blk * rows) ** 2 // 2
    d_spec = pl.BlockSpec((n_blk, 1, rows, cols), lambda b, h: (0, b, 0, 0))
    q_spec, k_spec, v_spec, lse_spec, tab_spec, w_spec, dw_spec = attention_specs(n_blk, rows, head, heads, group)
    return pl.pallas_call(
        functools.partial(bwd_kernel, group, heads, len(deps)),
        grid=(batch, heads),
        in_specs=[q_spec, k_spec, v_spec, q_spec, lse_spec, tab_spec, tab_spec, w_spec, w_spec] + [pl.BlockSpec(memory_space=pl.ANY)] * len(deps),
        out_specs=[d_spec, dw_spec, dw_spec],
        out_shape=[jax.ShapeDtypeStruct(qkv.shape, jnp.bfloat16),
                   jax.ShapeDtypeStruct((8, head), jnp.float32),
                   jax.ShapeDtypeStruct((8, head), jnp.float32)],
        scratch_shapes=[pltpu.VMEM((n_blk, 1, rows, head), jnp.bfloat16), pltpu.VMEM((n_blk * rows, head), jnp.float32), pltpu.VMEM((n_blk * rows, head), jnp.float32)],
        compiler_params=kernel_params(),
        cost_estimate=pl.CostEstimate(flops=pairs * head * 10, bytes_accessed=batch * n_blk * rows * 6000, transcendentals=pairs),
        name='attention_bwd',
    )(qkv, qkv, qkv, d_out, lse, cos_t, sin_t, wq, wk, *deps)


def copy_kernel(src_ref, dst_ref):
    dst_ref[...] = src_ref[...]


def settle(arr):
    rows, cols = arr.shape
    spec = pl.BlockSpec((256, cols), lambda i: (i, 0))
    return pl.pallas_call(
        copy_kernel, grid=(rows // 256,), in_specs=[spec], out_specs=spec,
        out_shape=jax.ShapeDtypeStruct(arr.shape, arr.dtype),
        cost_estimate=pl.CostEstimate(flops=rows * cols * 400, bytes_accessed=rows * cols * 4, transcendentals=0),
        name='settle',
    )(arr)


def split_kernel(n_dev, src_ref, k_ref, v_ref):
    half = k_ref.shape[1] // n_dev
    for j in range(n_dev):
        k_ref[:, j * half:(j + 1) * half] = src_ref[:, 2 * j * half:(2 * j + 1) * half]
        v_ref[:, j * half:(j + 1) * half] = src_ref[:, (2 * j + 1) * half:(2 * j + 2) * half]


def split_kv(arr, n_dev):
    rows, cols = arr.shape
    out = pl.BlockSpec((256, cols // 2), lambda i: (i, 0))
    shape = jax.ShapeDtypeStruct((rows, cols // 2), arr.dtype)
    return pl.pallas_call(
        functools.partial(split_kernel, n_dev), grid=(rows // 256,),
        in_specs=[pl.BlockSpec((256, cols), lambda i: (i, 0))], out_specs=[out, out], out_shape=[shape, shape],
        cost_estimate=pl.CostEstimate(flops=rows * cols * 400, bytes_accessed=rows * cols * 4, transcendentals=0),
        name='split_kv',
    )(arr)


def ein(spec, a, b):
    return jnp.einsum(spec, a, b, preferred_element_type=jnp.float32)


def solution(mesh):
    n_dev = mesh.shape['sp']

    def swap(arr):
        return lax.all_to_all(arr, 'sp', 0, 0, tiled=True)

    def gather(arr):
        return lax.all_gather(arr, 'sp', axis=0, tiled=False)

    def join(arr):
        n_blk, batch, rows, cols = arr.shape
        return jnp.transpose(arr, (1, 2, 0, 3)).reshape(batch, rows, n_blk * cols)

    def layer(x_in, dy_in, positions, w_q, w_k, w_v, w_o, w_pre, w_post, q_norm, k_norm):
        head = q_norm.shape[0]
        q_cols = w_q.shape[1] // n_dev
        kv_cols = w_k.shape[1] // n_dev
        heads = q_cols // head
        group = q_cols // kv_cols
        me = lax.axis_index('sp')
        bounds = []
        at = 0
        for size in CHUNKS:
            bounds.append((at, at + size))
            at += size
        parts = range(len(bounds))

        x_f32 = [x_in[lo:hi].astype(jnp.float32) for lo, hi in bounds]
        pre = [jax.vjp(pre_norm, x, w_pre) for x in x_f32]
        normed = [gather(pre[c][0]) for c in parts]
        cos_t, sin_t = rope_tables(lax.all_gather(positions, 'sp', axis=0, tiled=True), head)
        cos_t = cos_t.reshape(n_dev, -1, head)
        sin_t = sin_t.reshape(n_dev, -1, head)
        w_loc = jnp.concatenate([lax.dynamic_slice_in_dim(w_q, me * q_cols, q_cols, 1),
                                 lax.dynamic_slice_in_dim(w_k, me * kv_cols, kv_cols, 1),
                                 lax.dynamic_slice_in_dim(w_v, me * kv_cols, kv_cols, 1)], axis=1)
        wo_loc = lax.dynamic_slice_in_dim(w_o, me * q_cols, q_cols, 0)
        wq_row = q_norm[None, :]
        wk_row = k_norm[None, :]

        qkv, o_loc, lse, y_parts, d_proj_all = [], [], [], [], []
        dw_post = 0.0
        d_c = None
        for c in parts:
            lo, hi = bounds[c]
            qkv.append(ein('jbsd,dn->jbsn', normed[c], w_loc).astype(jnp.bfloat16))
            o_c, lse_c = attention_fwd(qkv[c], cos_t, sin_t, wq_row, wk_row, heads, group)
            o_loc.append(o_c)
            lse.append(lse_c)
            o_tok = swap(o_c)
            proj = ein('bsn,nd->bsd', join(o_tok), w_o).astype(jnp.bfloat16)
            post, post_pull = jax.vjp(post_norm, proj, w_post)
            y_parts.append((x_f32[c] + post).astype(jnp.bfloat16))
            d_c, dwp = post_pull(dy_in[lo:hi].astype(jnp.float32))
            dw_post = dw_post + dwp
            d_proj_all.append(gather(d_c))

        d_tok, d_head = [], []
        dw_o = 0.0
        dq_norm = 0.0
        dk_norm = 0.0
        last = len(bounds) - 1
        for c in parts:
            dw_o = dw_o + ein('jbsn,jbsd->nd', o_loc[c], d_proj_all[c])
            deps = (d_head[c - 1],) if c else (d_c,)
            if c == last:
                dw_o = dw_o.astype(jnp.bfloat16)
                deps += (dw_o,)
            d_o = ein('jbsd,nd->jbsn', d_proj_all[c], wo_loc).astype(jnp.bfloat16)
            d_qkv, dwq, dwk = attention_bwd(qkv[c], d_o, lse[c], cos_t, sin_t, wq_row, wk_row, heads, group, deps)
            dq_norm = dq_norm + jnp.sum(dwq, axis=0)
            dk_norm = dk_norm + jnp.sum(dwk, axis=0)
            d_head.append(d_qkv)
            d_tok.append(swap(d_qkv))

        def gather_to(axis):
            return lambda arr: lax.all_gather(arr, 'sp', axis=axis, tiled=True)

        dw_o = settle(gather_to(0)(dw_o))
        dw_q = sum(ein('jbsd,jbsn->dn', normed[c], d_head[c][..., :q_cols]) for c in parts).astype(jnp.bfloat16)
        dw_q = settle(gather_to(1)(dw_q))
        dw_kv = sum(ein('jbsd,jbsn->dn', normed[c], d_head[c][..., q_cols:]) for c in parts).astype(jnp.bfloat16)
        dw_k, dw_v = split_kv(gather_to(1)(dw_kv), n_dev)

        dx_parts = []
        dw_pre = 0.0
        for c in parts:
            lo, hi = bounds[c]
            dq = join(d_tok[c][..., :q_cols])
            dk = join(d_tok[c][..., q_cols:q_cols + kv_cols])
            dv = join(d_tok[c][..., q_cols + kv_cols:])
            d_normed = (ein('bsn,dn->bsd', dq, w_q) + ein('bsn,dn->bsd', dk, w_k) + ein('bsn,dn->bsd', dv, w_v)).astype(jnp.bfloat16)
            dx_norm, dwp = pre[c][1](d_normed)
            dw_pre = dw_pre + dwp
            dx_parts.append((dy_in[lo:hi].astype(jnp.float32) + dx_norm).astype(jnp.bfloat16))

        sums = lax.psum((dw_pre, dw_post, dq_norm, dk_norm), 'sp')
        return (jnp.concatenate(y_parts, axis=0), jnp.concatenate(dx_parts, axis=0), dw_q, dw_k, dw_v, dw_o) + sums

    token_spec = P('dp', 'sp', None)
    return jax.shard_map(layer, mesh=mesh,
                         in_specs=(token_spec, token_spec, P(('dp', 'sp')), P(None, None), P(None, None), P(None, None), P(None, None), P(None), P(None), P(None), P(None)),
                         out_specs=(token_spec, token_spec, P('dp', None), P('dp', None), P('dp', None), P('dp', None), P('dp'), P('dp'), P('dp'), P('dp')),
                         check_vma=False)
```

```python
import functools
import jax
import jax.numpy as jnp
from jax import lax
from jax.experimental import pallas as pl
from jax.experimental.pallas import tpu as pltpu
from jax.sharding import PartitionSpec as P

EPS = 1e-6
ROPE_BASE = 1000000.0
ROPE_SCALE = 8.0
NEG_BIG = -1e30
LOG2E = 1.4426950408889634
NORM_CHUNKS = (2, 2)
GRAD_CHUNKS = (2, 1, 1)


def rms_scale(x_f32, weight):
    inv_rms = lax.rsqrt(jnp.mean(x_f32 * x_f32, axis=-1, keepdims=True) + EPS)
    return x_f32 * inv_rms * (1.0 + weight)


def pre_norm(x_f32, weight):
    return rms_scale(x_f32, weight).astype(jnp.bfloat16)


def post_norm(proj, weight):
    return rms_scale(proj.astype(jnp.float32), weight)


def rope_tables(positions, head):
    half_dim = head // 2
    inv_freq = ROPE_BASE ** (-jnp.arange(half_dim, dtype=jnp.float32) * 2.0 / head)
    angles = (positions.astype(jnp.float32) / ROPE_SCALE)[:, None] * inv_freq[None, :]
    cosines = jnp.cos(angles)
    sines = jnp.sin(angles)
    return jnp.concatenate([cosines, cosines], axis=-1), jnp.concatenate([-sines, sines], axis=-1)


def dot_nt(a, b):
    return lax.dot_general(a, b, (((1,), (1,)), ((), ())), preferred_element_type=jnp.float32)


def dot_tn(a, b):
    return lax.dot_general(a, b, (((0,), (0,)), ((), ())), preferred_element_type=jnp.float32)


def dot_nn(a, b):
    return lax.dot_general(a, b, (((1,), (0,)), ((), ())), preferred_element_type=jnp.float32)


def rotate(x_bf, weight, cos_t, sin_t):
    normed = rms_scale(x_bf.astype(jnp.float32), weight)
    return (normed * cos_t + pltpu.roll(normed, normed.shape[-1] // 2, 1) * sin_t).astype(jnp.bfloat16)


def rotate_bwd(d_rot, x_bf, weight, cos_t, sin_t):
    d_f32 = d_rot.astype(jnp.float32)
    d_norm = d_f32 * cos_t - pltpu.roll(d_f32, d_f32.shape[-1] // 2, 1) * sin_t
    x = x_bf.astype(jnp.float32)
    inv_rms = lax.rsqrt(jnp.mean(x * x, axis=-1, keepdims=True) + EPS)
    unit = x * inv_rms
    scaled = d_norm * (1.0 + weight)
    dx = (scaled - unit * jnp.mean(scaled * unit, axis=-1, keepdims=True)) * inv_rms
    d_weight = jnp.sum((d_norm * unit).reshape(-1, 8, x.shape[-1]), axis=0)
    return dx.astype(jnp.bfloat16), d_weight


def causal(scores, fill):
    row_ids = lax.broadcasted_iota(jnp.int32, scores.shape, 0)
    col_ids = lax.broadcasted_iota(jnp.int32, scores.shape, 1)
    return jnp.where(row_ids >= col_ids, scores, fill)


def prefix(ref, count):
    block = ref[:count, 0]
    return block.reshape(count * block.shape[1], block.shape[2])


def fwd_kernel(group, q_ref, k_ref, v_ref, cos_ref, sin_ref, wq_ref, wk_ref, o_ref, lse_ref, k_rot):
    n_blk, _, rows, head = q_ref.shape
    member = lax.rem(pl.program_id(1), group)
    coef = head ** -0.5 * LOG2E
    wq = wq_ref[...]

    @pl.when(member == 0)
    def _():
        for j in range(n_blk):
            k_rot[j, 0] = rotate(k_ref[j, 0], wk_ref[...], cos_ref[j], sin_ref[j])

    for j in range(n_blk):
        q_rot = rotate(q_ref[j, 0], wq, cos_ref[j], sin_ref[j])
        s_diag = causal(dot_nt(q_rot, k_rot[j, 0]), NEG_BIG)
        row_max = jnp.max(s_diag, axis=-1, keepdims=True)
        if j:
            s_off = dot_nt(q_rot, prefix(k_rot, j))
            row_max = jnp.maximum(row_max, jnp.max(s_off, axis=-1, keepdims=True))
        e_diag = jnp.exp2((s_diag - row_max) * coef)
        row_sum = jnp.sum(e_diag, axis=-1, keepdims=True)
        if j:
            e_off = jnp.exp2((s_off - row_max) * coef)
            row_sum = row_sum + jnp.sum(e_off, axis=-1, keepdims=True)
        inv_sum = 1.0 / row_sum
        out = dot_nn((e_diag * inv_sum).astype(jnp.bfloat16), v_ref[j, 0])
        if j:
            out = out + dot_nn((e_off * inv_sum).astype(jnp.bfloat16), prefix(v_ref, j))
        o_ref[j, 0] = out.astype(jnp.bfloat16)
        lse = jnp.broadcast_to(row_max * coef + jnp.log2(row_sum), (rows, head))
        lanes = lax.broadcasted_iota(jnp.int32, (rows, head), 1)
        owner = lax.div(lanes, head // group)
        lse_ref[0, 0, j] = jnp.where(owner >= member, lse, lse_ref[0, 0, j])


def bwd_kernel(group, heads, n_deps, q_ref, k_ref, v_ref, do_ref, lse_ref, cos_ref, sin_ref, wq_ref, wk_ref, *refs):
    d_ref, dwq_ref, dwk_ref, k_rot, dk_acc, dv_acc = refs[n_deps:]
    n_blk, _, rows, head = q_ref.shape
    member = lax.rem(pl.program_id(1), group)
    pair = lax.div(pl.program_id(1), group)
    q_lanes = pl.ds(pl.multiple_of(pl.program_id(1) * head, head), head)
    k_lanes = pl.ds(pl.multiple_of((heads + pair) * head, head), head)
    v_lanes = pl.ds(pl.multiple_of((heads + heads // group + pair) * head, head), head)
    scale = head ** -0.5
    coef = scale * LOG2E
    wq = wq_ref[...]
    wk = wk_ref[...]

    @pl.when(jnp.logical_and(pl.program_id(0) == 0, pl.program_id(1) == 0))
    def _():
        dwq_ref[...] = jnp.zeros_like(dwq_ref)
        dwk_ref[...] = jnp.zeros_like(dwk_ref)

    @pl.when(member == 0)
    def _():
        dk_acc[...] = jnp.zeros_like(dk_acc)
        dv_acc[...] = jnp.zeros_like(dv_acc)
        for j in range(n_blk):
            k_rot[j, 0] = rotate(k_ref[j, 0], wk, cos_ref[j], sin_ref[j])

    for j in range(n_blk):
        here = slice(j * rows, (j + 1) * rows)
        before = slice(0, j * rows)
        q_raw = q_ref[j, 0]
        q_rot = rotate(q_raw, wq, cos_ref[j], sin_ref[j])
        d_out = do_ref[j, 0]
        lse_all = lse_ref[0, 0, j]
        lse = lse_all[:, :1]
        for other in range(1, group):
            at = other * (head // group)
            lse = jnp.where(member == other, lse_all[:, at:at + 1], lse)
        p_diag = causal(jnp.exp2(dot_nt(q_rot, k_rot[j, 0]) * coef - lse), 0.0)
        dp_diag = dot_nt(d_out, v_ref[j, 0])
        delta = jnp.sum(p_diag * dp_diag, axis=-1, keepdims=True)
        if j:
            p_off = jnp.exp2(dot_nt(q_rot, prefix(k_rot, j)) * coef - lse)
            dp_off = dot_nt(d_out, prefix(v_ref, j))
            delta = delta + jnp.sum(p_off * dp_off, axis=-1, keepdims=True)
        ds_diag = (p_diag * (dp_diag - delta) * scale).astype(jnp.bfloat16)
        dq = dot_nn(ds_diag, k_rot[j, 0])
        dk_acc[here, :] += dot_tn(ds_diag, q_rot)
        dv_acc[here, :] += dot_tn(p_diag.astype(jnp.bfloat16), d_out)
        if j:
            ds_off = (p_off * (dp_off - delta) * scale).astype(jnp.bfloat16)
            dq = dq + dot_nn(ds_off, prefix(k_rot, j))
            dk_acc[before, :] += dot_tn(ds_off, q_rot)
            dv_acc[before, :] += dot_tn(p_off.astype(jnp.bfloat16), d_out)
        d_ref[j, 0, :, q_lanes], dw = rotate_bwd(dq.astype(jnp.bfloat16), q_raw, wq, cos_ref[j], sin_ref[j])
        dwq_ref[...] += dw

    @pl.when(member == group - 1)
    def _():
        for j in range(n_blk):
            here = slice(j * rows, (j + 1) * rows)
            d_ref[j, 0, :, k_lanes], dw = rotate_bwd(dk_acc[here, :].astype(jnp.bfloat16), k_ref[j, 0], wk, cos_ref[j], sin_ref[j])
            dwk_ref[...] += dw
            d_ref[j, 0, :, v_lanes] = dv_acc[here, :].astype(jnp.bfloat16)


def attention_specs(n_blk, rows, head, heads, group, first, do_first=0):
    kv = heads // group
    block = (n_blk, 1, rows, head)
    o_spec = pl.BlockSpec(block, lambda b, h: (0, do_first + b, 0, h))
    q_spec = pl.BlockSpec(block, lambda b, h: (0, first + b, 0, h))
    k_spec = pl.BlockSpec(block, lambda b, h: (0, first + b, 0, heads + h // group))
    v_spec = pl.BlockSpec(block, lambda b, h: (0, first + b, 0, heads + kv + h // group))
    lse_spec = pl.BlockSpec((1, 1, n_blk, rows, head), lambda b, h: (b, h // group, 0, 0, 0))
    tab_spec = pl.BlockSpec((n_blk, rows, head), lambda b, h: (0, 0, 0))
    w_spec = pl.BlockSpec((1, head), lambda b, h: (0, 0))
    dw_spec = pl.BlockSpec((8, head), lambda b, h: (0, 0))
    return o_spec, q_spec, k_spec, v_spec, lse_spec, tab_spec, w_spec, dw_spec


def kernel_params():
    return pltpu.CompilerParams(dimension_semantics=('arbitrary', 'arbitrary'), vmem_limit_bytes=56 * 2 ** 20)


def attention_fwd(qkv, first, cos_t, sin_t, wq, wk, heads, group):
    n_blk, _, rows, _ = qkv.shape
    batch = 1
    head = cos_t.shape[2]
    pairs = batch * heads * (n_blk * rows) ** 2 // 2
    o_spec, q_spec, k_spec, v_spec, lse_spec, tab_spec, w_spec, _ = attention_specs(n_blk, rows, head, heads, group, first)
    return pl.pallas_call(
        functools.partial(fwd_kernel, group),
        grid=(batch, heads),
        in_specs=[q_spec, k_spec, v_spec, tab_spec, tab_spec, w_spec, w_spec],
        out_specs=[o_spec, lse_spec],
        out_shape=[jax.ShapeDtypeStruct((n_blk, batch, rows, heads * head), jnp.bfloat16),
                   jax.ShapeDtypeStruct((batch, heads // group, n_blk, rows, head), jnp.float32)],
        scratch_shapes=[pltpu.VMEM((n_blk, 1, rows, head), jnp.bfloat16)],
        compiler_params=kernel_params(),
        cost_estimate=pl.CostEstimate(flops=pairs * head * 4, bytes_accessed=batch * n_blk * rows * 3000, transcendentals=pairs),
        name='attention_fwd',
    )(qkv, qkv, qkv, cos_t, sin_t, wq, wk)


def attention_bwd(qkv, first, d_out, do_first, lse, cos_t, sin_t, wq, wk, heads, group, deps=()):
    n_blk, _, rows, cols = qkv.shape
    batch = 1
    head = cos_t.shape[2]
    pairs = batch * heads * (n_blk * rows) ** 2 // 2
    d_spec = pl.BlockSpec((n_blk, 1, rows, cols), lambda b, h: (0, b, 0, 0))
    o_spec, q_spec, k_spec, v_spec, lse_spec, tab_spec, w_spec, dw_spec = attention_specs(n_blk, rows, head, heads, group, first, do_first)
    return pl.pallas_call(
        functools.partial(bwd_kernel, group, heads, len(deps)),
        grid=(batch, heads),
        in_specs=[q_spec, k_spec, v_spec, o_spec, lse_spec, tab_spec, tab_spec, w_spec, w_spec] + [pl.BlockSpec(memory_space=pl.ANY)] * len(deps),
        out_specs=[d_spec, dw_spec, dw_spec],
        out_shape=[jax.ShapeDtypeStruct((n_blk, batch, rows, cols), jnp.bfloat16),
                   jax.ShapeDtypeStruct((8, head), jnp.float32),
                   jax.ShapeDtypeStruct((8, head), jnp.float32)],
        scratch_shapes=[pltpu.VMEM((n_blk, 1, rows, head), jnp.bfloat16), pltpu.VMEM((n_blk * rows, head), jnp.float32), pltpu.VMEM((n_blk * rows, head), jnp.float32)],
        compiler_params=kernel_params(),
        cost_estimate=pl.CostEstimate(flops=pairs * head * 10, bytes_accessed=batch * n_blk * rows * 6000, transcendentals=pairs),
        name='attention_bwd',
    )(qkv, qkv, qkv, d_out, lse, cos_t, sin_t, wq, wk, *deps)


def copy_kernel(src_ref, dst_ref):
    dst_ref[...] = src_ref[...]


def settle(arr, steps):
    rows, cols = arr.shape
    spec = pl.BlockSpec((rows // steps, cols), lambda i: (i, 0))
    return pl.pallas_call(
        copy_kernel, grid=(steps,), compiler_params=pltpu.CompilerParams(vmem_limit_bytes=56 * 2 ** 20), in_specs=[spec], out_specs=spec,
        out_shape=jax.ShapeDtypeStruct(arr.shape, arr.dtype),
        cost_estimate=pl.CostEstimate(flops=rows * cols * 400, bytes_accessed=rows * cols * 4, transcendentals=0),
        name='settle',
    )(arr)


def split_kernel(n_dev, src_ref, q_ref, k_ref):
    q_cols = q_ref.shape[1] // n_dev
    k_cols = k_ref.shape[1] // n_dev
    for j in range(n_dev):
        at = j * (q_cols + k_cols)
        q_ref[:, j * q_cols:(j + 1) * q_cols] = src_ref[:, at:at + q_cols]
        k_ref[:, j * k_cols:(j + 1) * k_cols] = src_ref[:, at + q_cols:at + q_cols + k_cols]


def split_qk(arr, n_dev, q_wide, k_wide, steps):
    rows, cols = arr.shape
    return pl.pallas_call(
        functools.partial(split_kernel, n_dev), grid=(steps,), compiler_params=pltpu.CompilerParams(vmem_limit_bytes=56 * 2 ** 20),
        in_specs=[pl.BlockSpec((rows // steps, cols), lambda i: (i, 0))],
        out_specs=[pl.BlockSpec((rows // steps, q_wide), lambda i: (i, 0)), pl.BlockSpec((rows // steps, k_wide), lambda i: (i, 0))],
        out_shape=[jax.ShapeDtypeStruct((rows, q_wide), arr.dtype), jax.ShapeDtypeStruct((rows, k_wide), arr.dtype)],
        cost_estimate=pl.CostEstimate(flops=rows * cols * 400, bytes_accessed=rows * cols * 4, transcendentals=0),
        name='split_qk',
    )(arr)


def ein(spec, a, b):
    return jnp.einsum(spec, a, b, preferred_element_type=jnp.float32)


AFTER_DWO = 2


def spans(sizes):
    ends = [sum(sizes[:i + 1]) for i in range(len(sizes))]
    return [(end - size, end) for size, end in zip(sizes, ends)]


def solution(mesh):
    n_dev = mesh.shape['sp']

    def swap(arr):
        return lax.all_to_all(arr, 'sp', 0, 0, tiled=True)

    def gather(arr):
        return lax.all_gather(arr, 'sp', axis=0, tiled=False)

    def join(arr):
        n_blk, batch, rows, cols = arr.shape
        return jnp.transpose(arr, (1, 2, 0, 3)).reshape(batch, rows, n_blk * cols)

    def layer(x_in, dy_in, positions, w_q, w_k, w_v, w_o, w_pre, w_post, q_norm, k_norm):
        head = q_norm.shape[0]
        q_cols = w_q.shape[1] // n_dev
        kv_cols = w_k.shape[1] // n_dev
        heads = q_cols // head
        group = q_cols // kv_cols
        me = lax.axis_index('sp')
        batch = x_in.shape[0]
        wide = spans(NORM_CHUNKS)
        steps = spans(GRAD_CHUNKS)
        seqs = range(batch)
        home = [next((g, i - lo) for g, (lo, hi) in enumerate(wide) if lo <= i < hi) for i in seqs]
        turn = [next((g, i - lo) for g, (lo, hi) in enumerate(steps) if lo <= i < hi) for i in seqs]

        x_f32 = [x_in[i:i + 1].astype(jnp.float32) for i in seqs]
        normed = [gather(pre_norm(x_in[lo:hi].astype(jnp.float32), w_pre)) for lo, hi in wide]
        cos_t, sin_t = rope_tables(lax.all_gather(positions, 'sp', axis=0, tiled=True), head)
        cos_t = cos_t.reshape(n_dev, -1, head)
        sin_t = sin_t.reshape(n_dev, -1, head)
        w_loc = jnp.concatenate([lax.dynamic_slice_in_dim(w_q, me * q_cols, q_cols, 1),
                                 lax.dynamic_slice_in_dim(w_k, me * kv_cols, kv_cols, 1),
                                 lax.dynamic_slice_in_dim(w_v, me * kv_cols, kv_cols, 1)], axis=1)
        wo_loc = lax.dynamic_slice_in_dim(w_o, me * q_cols, q_cols, 0)
        wq_row = q_norm[None, :]
        wk_row = k_norm[None, :]

        o_tok, qkv, o_loc, lse, y_parts, d_parts, d_proj_all = [], [], [], [], [], [], []
        dw_post = 0.0
        for i in seqs:
            g, first = home[i]
            if not first:
                qkv.append(ein('jbsd,dn->jbsn', normed[g], w_loc).astype(jnp.bfloat16))
            o_i, lse_i = attention_fwd(qkv[g], first, cos_t, sin_t, wq_row, wk_row, heads, group)
            o_loc.append(o_i)
            lse.append(lse_i)
            o_tok.append(swap(o_i))
            proj = ein('bsn,nd->bsd', join(o_tok[i]), w_o).astype(jnp.bfloat16)
            if i:
                proj, _ = lax.optimization_barrier((proj, d_parts[-1]))
            post, post_pull = jax.vjp(post_norm, proj, w_post)
            d_i, dwp = post_pull(dy_in[i:i + 1].astype(jnp.float32))
            dw_post = dw_post + dwp
            d_parts.append(d_i)
            y_parts.append((x_f32[i] + post).astype(jnp.bfloat16))
            step, _ = turn[i]
            lo, hi = steps[step]
            own = d_parts[lo:] if hi - lo == 1 else [jnp.concatenate(d_parts[lo:], axis=0)]
            if i + 1 == hi:
                d_proj_all.append(gather(own[0]))

        d_o = []
        dw_o = 0.0
        for step, (lo, hi) in enumerate(steps):
            for k in range(lo, hi):
                d_k = d_proj_all[step] if hi - lo == 1 else d_proj_all[step][:, k - lo:k - lo + 1]
                dw_o = dw_o + ein('jbsn,jbsd->nd', o_loc[k], d_k)
            dw_o = dw_o.astype(jnp.bfloat16) if hi == batch else lax.optimization_barrier(dw_o)
            d_o.append(ein('jbsd,nd->jbsn', d_proj_all[step], wo_loc).astype(jnp.bfloat16))

        d_tok, d_head = [], []
        dq_norm = 0.0
        dk_norm = 0.0
        for i in seqs:
            g, first = home[i]
            step, place = turn[i]
            deps = (d_head[i - 1],) if i else (d_parts[-1],)
            if i == AFTER_DWO:
                deps += (dw_o,)
            d_qkv, dwq, dwk = attention_bwd(qkv[g], first, d_o[step], place, lse[i], cos_t, sin_t, wq_row, wk_row, heads, group, deps)
            dq_norm = dq_norm + jnp.sum(dwq, axis=0)
            dk_norm = dk_norm + jnp.sum(dwk, axis=0)
            d_head.append(d_qkv)
            d_tok.append(swap(d_qkv))

        def gather_to(axis):
            return lambda arr: lax.all_gather(arr, 'sp', axis=axis, tiled=True)

        dw_o = settle(gather_to(0)(dw_o), 8)
        qk = q_cols + kv_cols
        dw_qk, dw_v = 0.0, 0.0
        for g in range(len(wide)):
            own = [d_head[i] for i in seqs if home[i][0] == g]
            for i, d in enumerate(own):
                n_g = normed[g] if len(own) == 1 else normed[g][:, i:i + 1]
                dw_qk = dw_qk + ein('jbsd,jbsn->dn', n_g, d[..., :qk])
            for i, d in enumerate(own):
                n_g = normed[g] if len(own) == 1 else normed[g][:, i:i + 1]
                dw_v = dw_v + ein('jbsd,jbsn->dn', n_g, d[..., qk:])
            if g == 0:
                dw_qk = lax.optimization_barrier(dw_qk)
                dw_v = lax.optimization_barrier(dw_v)
        dw_q, dw_k = split_qk(gather_to(1)(dw_qk.astype(jnp.bfloat16)), n_dev, w_q.shape[1], w_k.shape[1], 9)
        dw_v = settle(gather_to(1)(dw_v.astype(jnp.bfloat16)), 6)

        dx_parts = []
        dw_pre = 0.0
        for lo, hi in wide:
            tok = jnp.concatenate(d_tok[lo:hi], axis=1)
            dq = join(tok[..., :q_cols])
            dk = join(tok[..., q_cols:qk])
            dv = join(tok[..., qk:])
            d_normed = (ein('bsn,dn->bsd', dq, w_q) + ein('bsn,dn->bsd', dk, w_k) + ein('bsn,dn->bsd', dv, w_v)).astype(jnp.bfloat16)
            dx_norm, dwp = jax.vjp(pre_norm, x_in[lo:hi].astype(jnp.float32), w_pre)[1](d_normed)
            dw_pre = dw_pre + dwp
            dx_parts.append((dy_in[lo:hi].astype(jnp.float32) + dx_norm).astype(jnp.bfloat16))

        sums = lax.psum((dw_pre, dw_post, dq_norm, dk_norm), 'sp')
        return (jnp.concatenate(y_parts, axis=0), jnp.concatenate(dx_parts, axis=0), dw_q, dw_k, dw_v, dw_o) + sums

    token_spec = P('dp', 'sp', None)
    return jax.shard_map(layer, mesh=mesh,
                         in_specs=(token_spec, token_spec, P(('dp', 'sp')), P(None, None), P(None, None), P(None, None), P(None, None), P(None), P(None), P(None), P(None)),
                         out_specs=(token_spec, token_spec, P('dp', None), P('dp', None), P('dp', None), P('dp', None), P('dp'), P('dp'), P('dp'), P('dp')),
                         check_vma=False)
```

```python
import functools
import jax
import jax.numpy as jnp
from jax import lax
from jax.experimental import pallas as pl
from jax.experimental.pallas import tpu as pltpu
from jax.sharding import PartitionSpec as P

EPS = 1e-6
ROPE_BASE = 1000000.0
ROPE_SCALE = 8.0
NEG_BIG = -1e30
LOG2E = 1.4426950408889634
NORM_CHUNKS = (2, 2)
GRAD_CHUNKS = (2, 1, 1)


def rms_scale(x_f32, weight):
    inv_rms = lax.rsqrt(jnp.mean(x_f32 * x_f32, axis=-1, keepdims=True) + EPS)
    return x_f32 * inv_rms * (1.0 + weight)


def pre_norm(x_f32, weight):
    return rms_scale(x_f32, weight).astype(jnp.bfloat16)


def post_norm(proj, weight):
    return rms_scale(proj.astype(jnp.float32), weight)


def rope_tables(positions, head):
    half_dim = head // 2
    inv_freq = ROPE_BASE ** (-jnp.arange(half_dim, dtype=jnp.float32) * 2.0 / head)
    angles = (positions.astype(jnp.float32) / ROPE_SCALE)[:, None] * inv_freq[None, :]
    cosines = jnp.cos(angles)
    sines = jnp.sin(angles)
    return jnp.concatenate([cosines, cosines], axis=-1), jnp.concatenate([-sines, sines], axis=-1)


def dot_nt(a, b):
    return lax.dot_general(a, b, (((1,), (1,)), ((), ())), preferred_element_type=jnp.float32)


def dot_tn(a, b):
    return lax.dot_general(a, b, (((0,), (0,)), ((), ())), preferred_element_type=jnp.float32)


def dot_nn(a, b):
    return lax.dot_general(a, b, (((1,), (0,)), ((), ())), preferred_element_type=jnp.float32)


def rotate(x_bf, weight, cos_t, sin_t):
    normed = rms_scale(x_bf.astype(jnp.float32), weight)
    return (normed * cos_t + pltpu.roll(normed, normed.shape[-1] // 2, 1) * sin_t).astype(jnp.bfloat16)


def rotate_bwd(d_rot, x_bf, weight, cos_t, sin_t):
    d_f32 = d_rot.astype(jnp.float32)
    d_norm = d_f32 * cos_t - pltpu.roll(d_f32, d_f32.shape[-1] // 2, 1) * sin_t
    x = x_bf.astype(jnp.float32)
    inv_rms = lax.rsqrt(jnp.mean(x * x, axis=-1, keepdims=True) + EPS)
    unit = x * inv_rms
    scaled = d_norm * (1.0 + weight)
    dx = (scaled - unit * jnp.mean(scaled * unit, axis=-1, keepdims=True)) * inv_rms
    d_weight = jnp.sum((d_norm * unit).reshape(-1, 8, x.shape[-1]), axis=0)
    return dx.astype(jnp.bfloat16), d_weight


def causal(scores, fill):
    row_ids = lax.broadcasted_iota(jnp.int32, scores.shape, 0)
    col_ids = lax.broadcasted_iota(jnp.int32, scores.shape, 1)
    return jnp.where(row_ids >= col_ids, scores, fill)


def prefix(ref, count):
    block = ref[:count, 0]
    return block.reshape(count * block.shape[1], block.shape[2])


def fwd_kernel(group, q_ref, k_ref, v_ref, cos_ref, sin_ref, wq_ref, wk_ref, o_ref, lse_ref, k_rot):
    n_blk, _, rows, head = q_ref.shape
    member = lax.rem(pl.program_id(1), group)
    coef = head ** -0.5 * LOG2E
    wq = wq_ref[...]

    @pl.when(member == 0)
    def _():
        for j in range(n_blk):
            k_rot[j, 0] = rotate(k_ref[j, 0], wk_ref[...], cos_ref[j], sin_ref[j])

    for j in range(n_blk):
        q_rot = rotate(q_ref[j, 0], wq, cos_ref[j], sin_ref[j])
        s_diag = causal(dot_nt(q_rot, k_rot[j, 0]), NEG_BIG)
        row_max = jnp.max(s_diag, axis=-1, keepdims=True)
        if j:
            s_off = dot_nt(q_rot, prefix(k_rot, j))
            row_max = jnp.maximum(row_max, jnp.max(s_off, axis=-1, keepdims=True))
        e_diag = jnp.exp2((s_diag - row_max) * coef)
        row_sum = jnp.sum(e_diag, axis=-1, keepdims=True)
        if j:
            e_off = jnp.exp2((s_off - row_max) * coef)
            row_sum = row_sum + jnp.sum(e_off, axis=-1, keepdims=True)
        inv_sum = 1.0 / row_sum
        out = dot_nn((e_diag * inv_sum).astype(jnp.bfloat16), v_ref[j, 0])
        if j:
            out = out + dot_nn((e_off * inv_sum).astype(jnp.bfloat16), prefix(v_ref, j))
        o_ref[j, 0] = out.astype(jnp.bfloat16)
        lse = jnp.broadcast_to(row_max * coef + jnp.log2(row_sum), (rows, head))
        lanes = lax.broadcasted_iota(jnp.int32, (rows, head), 1)
        owner = lax.div(lanes, head // group)
        lse_ref[0, 0, j] = jnp.where(owner >= member, lse, lse_ref[0, 0, j])


def bwd_kernel(group, heads, n_deps, q_ref, k_ref, v_ref, do_ref, lse_ref, cos_ref, sin_ref, wq_ref, wk_ref, *refs):
    d_ref, dwq_ref, dwk_ref, k_rot, dk_acc, dv_acc = refs[n_deps:]
    n_blk, _, rows, head = q_ref.shape
    member = lax.rem(pl.program_id(1), group)
    pair = lax.div(pl.program_id(1), group)
    q_lanes = pl.ds(pl.multiple_of(pl.program_id(1) * head, head), head)
    k_lanes = pl.ds(pl.multiple_of((heads + pair) * head, head), head)
    v_lanes = pl.ds(pl.multiple_of((heads + heads // group + pair) * head, head), head)
    scale = head ** -0.5
    coef = scale * LOG2E
    wq = wq_ref[...]
    wk = wk_ref[...]

    @pl.when(jnp.logical_and(pl.program_id(0) == 0, pl.program_id(1) == 0))
    def _():
        dwq_ref[...] = jnp.zeros_like(dwq_ref)
        dwk_ref[...] = jnp.zeros_like(dwk_ref)

    @pl.when(member == 0)
    def _():
        dk_acc[...] = jnp.zeros_like(dk_acc)
        dv_acc[...] = jnp.zeros_like(dv_acc)
        for j in range(n_blk):
            k_rot[j, 0] = rotate(k_ref[j, 0], wk, cos_ref[j], sin_ref[j])

    for j in range(n_blk):
        here = slice(j * rows, (j + 1) * rows)
        before = slice(0, j * rows)
        q_raw = q_ref[j, 0]
        q_rot = rotate(q_raw, wq, cos_ref[j], sin_ref[j])
        d_out = do_ref[j, 0]
        lse_all = lse_ref[0, 0, j]
        lse = lse_all[:, :1]
        for other in range(1, group):
            at = other * (head // group)
            lse = jnp.where(member == other, lse_all[:, at:at + 1], lse)
        p_diag = causal(jnp.exp2(dot_nt(q_rot, k_rot[j, 0]) * coef - lse), 0.0)
        dp_diag = dot_nt(d_out, v_ref[j, 0])
        delta = jnp.sum(p_diag * dp_diag, axis=-1, keepdims=True)
        if j:
            p_off = jnp.exp2(dot_nt(q_rot, prefix(k_rot, j)) * coef - lse)
            dp_off = dot_nt(d_out, prefix(v_ref, j))
            delta = delta + jnp.sum(p_off * dp_off, axis=-1, keepdims=True)
        ds_diag = (p_diag * (dp_diag - delta) * scale).astype(jnp.bfloat16)
        dq = dot_nn(ds_diag, k_rot[j, 0])
        dk_acc[here, :] += dot_tn(ds_diag, q_rot)
        dv_acc[here, :] += dot_tn(p_diag.astype(jnp.bfloat16), d_out)
        if j:
            ds_off = (p_off * (dp_off - delta) * scale).astype(jnp.bfloat16)
            dq = dq + dot_nn(ds_off, prefix(k_rot, j))
            dk_acc[before, :] += dot_tn(ds_off, q_rot)
            dv_acc[before, :] += dot_tn(p_off.astype(jnp.bfloat16), d_out)
        d_ref[j, 0, :, q_lanes], dw = rotate_bwd(dq.astype(jnp.bfloat16), q_raw, wq, cos_ref[j], sin_ref[j])
        dwq_ref[...] += dw

    @pl.when(member == group - 1)
    def _():
        for j in range(n_blk):
            here = slice(j * rows, (j + 1) * rows)
            d_ref[j, 0, :, k_lanes], dw = rotate_bwd(dk_acc[here, :].astype(jnp.bfloat16), k_ref[j, 0], wk, cos_ref[j], sin_ref[j])
            dwk_ref[...] += dw
            d_ref[j, 0, :, v_lanes] = dv_acc[here, :].astype(jnp.bfloat16)


def attention_specs(n_blk, rows, head, heads, group, first, do_first=0):
    kv = heads // group
    block = (n_blk, 1, rows, head)
    o_spec = pl.BlockSpec(block, lambda b, h: (0, do_first + b, 0, h))
    q_spec = pl.BlockSpec(block, lambda b, h: (0, first + b, 0, h))
    k_spec = pl.BlockSpec(block, lambda b, h: (0, first + b, 0, heads + h // group))
    v_spec = pl.BlockSpec(block, lambda b, h: (0, first + b, 0, heads + kv + h // group))
    lse_spec = pl.BlockSpec((1, 1, n_blk, rows, head), lambda b, h: (b, h // group, 0, 0, 0))
    tab_spec = pl.BlockSpec((n_blk, rows, head), lambda b, h: (0, 0, 0))
    w_spec = pl.BlockSpec((1, head), lambda b, h: (0, 0))
    dw_spec = pl.BlockSpec((8, head), lambda b, h: (0, 0))
    return o_spec, q_spec, k_spec, v_spec, lse_spec, tab_spec, w_spec, dw_spec


def kernel_params():
    return pltpu.CompilerParams(dimension_semantics=('arbitrary', 'arbitrary'), vmem_limit_bytes=56 * 2 ** 20)


def attention_fwd(qkv, first, cos_t, sin_t, wq, wk, heads, group):
    n_blk, _, rows, _ = qkv.shape
    batch = 1
    head = cos_t.shape[2]
    pairs = batch * heads * (n_blk * rows) ** 2 // 2
    o_spec, q_spec, k_spec, v_spec, lse_spec, tab_spec, w_spec, _ = attention_specs(n_blk, rows, head, heads, group, first)
    return pl.pallas_call(
        functools.partial(fwd_kernel, group),
        grid=(batch, heads),
        in_specs=[q_spec, k_spec, v_spec, tab_spec, tab_spec, w_spec, w_spec],
        out_specs=[o_spec, lse_spec],
        out_shape=[jax.ShapeDtypeStruct((n_blk, batch, rows, heads * head), jnp.bfloat16),
                   jax.ShapeDtypeStruct((batch, heads // group, n_blk, rows, head), jnp.float32)],
        scratch_shapes=[pltpu.VMEM((n_blk, 1, rows, head), jnp.bfloat16)],
        compiler_params=kernel_params(),
        cost_estimate=pl.CostEstimate(flops=pairs * head * 4, bytes_accessed=batch * n_blk * rows * 3000, transcendentals=pairs),
        name='attention_fwd',
    )(qkv, qkv, qkv, cos_t, sin_t, wq, wk)


def attention_bwd(qkv, first, d_out, do_first, lse, cos_t, sin_t, wq, wk, heads, group, deps=()):
    n_blk, _, rows, cols = qkv.shape
    batch = 1
    head = cos_t.shape[2]
    pairs = batch * heads * (n_blk * rows) ** 2 // 2
    d_spec = pl.BlockSpec((n_blk, 1, rows, cols), lambda b, h: (0, b, 0, 0))
    o_spec, q_spec, k_spec, v_spec, lse_spec, tab_spec, w_spec, dw_spec = attention_specs(n_blk, rows, head, heads, group, first, do_first)
    return pl.pallas_call(
        functools.partial(bwd_kernel, group, heads, len(deps)),
        grid=(batch, heads),
        in_specs=[q_spec, k_spec, v_spec, o_spec, lse_spec, tab_spec, tab_spec, w_spec, w_spec] + [pl.BlockSpec(memory_space=pl.ANY)] * len(deps),
        out_specs=[d_spec, dw_spec, dw_spec],
        out_shape=[jax.ShapeDtypeStruct((n_blk, batch, rows, cols), jnp.bfloat16),
                   jax.ShapeDtypeStruct((8, head), jnp.float32),
                   jax.ShapeDtypeStruct((8, head), jnp.float32)],
        scratch_shapes=[pltpu.VMEM((n_blk, 1, rows, head), jnp.bfloat16), pltpu.VMEM((n_blk * rows, head), jnp.float32), pltpu.VMEM((n_blk * rows, head), jnp.float32)],
        compiler_params=kernel_params(),
        cost_estimate=pl.CostEstimate(flops=pairs * head * 10, bytes_accessed=batch * n_blk * rows * 6000, transcendentals=pairs),
        name='attention_bwd',
    )(qkv, qkv, qkv, d_out, lse, cos_t, sin_t, wq, wk, *deps)


def norm_kernel(x_ref, w_ref, out_ref):
    out_ref[...] = pre_norm(x_ref[...].astype(jnp.float32), w_ref[...])


def pre_norm_rows(x, weight, lo, hi):
    batch = hi - lo
    _, rows, width = x.shape
    return pl.pallas_call(
        norm_kernel, grid=(batch, 2),
        in_specs=[pl.BlockSpec((1, rows // 2, width), lambda b, i: (lo + b, i, 0)), pl.BlockSpec((1, width), lambda b, i: (0, 0))],
        out_specs=pl.BlockSpec((1, rows // 2, width), lambda b, i: (b, i, 0)),
        out_shape=jax.ShapeDtypeStruct((batch, rows, width), jnp.bfloat16),
        compiler_params=pltpu.CompilerParams(vmem_limit_bytes=60 * 2 ** 20),
        cost_estimate=pl.CostEstimate(flops=batch * rows * width * 8, bytes_accessed=batch * rows * width * 4, transcendentals=0),
        name='pre_norm',
    )(x, weight[None, :])


def copy_kernel(src_ref, dst_ref):
    dst_ref[...] = src_ref[...]


def settle(arr, steps):
    rows, cols = arr.shape
    spec = pl.BlockSpec((rows // steps, cols), lambda i: (i, 0))
    return pl.pallas_call(
        copy_kernel, grid=(steps,), compiler_params=pltpu.CompilerParams(vmem_limit_bytes=56 * 2 ** 20), in_specs=[spec], out_specs=spec,
        out_shape=jax.ShapeDtypeStruct(arr.shape, arr.dtype),
        cost_estimate=pl.CostEstimate(flops=rows * cols * 400, bytes_accessed=rows * cols * 4, transcendentals=0),
        name='settle',
    )(arr)


def split_kernel(n_dev, src_ref, q_ref, k_ref):
    q_cols = q_ref.shape[1] // n_dev
    k_cols = k_ref.shape[1] // n_dev
    for j in range(n_dev):
        at = j * (q_cols + k_cols)
        q_ref[:, j * q_cols:(j + 1) * q_cols] = src_ref[:, at:at + q_cols]
        k_ref[:, j * k_cols:(j + 1) * k_cols] = src_ref[:, at + q_cols:at + q_cols + k_cols]


def split_qk(arr, n_dev, q_wide, k_wide, steps):
    rows, cols = arr.shape
    return pl.pallas_call(
        functools.partial(split_kernel, n_dev), grid=(steps,), compiler_params=pltpu.CompilerParams(vmem_limit_bytes=56 * 2 ** 20),
        in_specs=[pl.BlockSpec((rows // steps, cols), lambda i: (i, 0))],
        out_specs=[pl.BlockSpec((rows // steps, q_wide), lambda i: (i, 0)), pl.BlockSpec((rows // steps, k_wide), lambda i: (i, 0))],
        out_shape=[jax.ShapeDtypeStruct((rows, q_wide), arr.dtype), jax.ShapeDtypeStruct((rows, k_wide), arr.dtype)],
        cost_estimate=pl.CostEstimate(flops=rows * cols * 400, bytes_accessed=rows * cols * 4, transcendentals=0),
        name='split_qk',
    )(arr)


def ein(spec, a, b):
    return jnp.einsum(spec, a, b, preferred_element_type=jnp.float32)


AFTER_DWO = 2


def spans(sizes):
    ends = [sum(sizes[:i + 1]) for i in range(len(sizes))]
    return [(end - size, end) for size, end in zip(sizes, ends)]


def solution(mesh):
    n_dev = mesh.shape['sp']

    def swap(arr):
        return lax.all_to_all(arr, 'sp', 0, 0, tiled=True)

    def gather(arr):
        return lax.all_gather(arr, 'sp', axis=0, tiled=False)

    def join(arr):
        n_blk, batch, rows, cols = arr.shape
        return jnp.transpose(arr, (1, 2, 0, 3)).reshape(batch, rows, n_blk * cols)

    def layer(x_in, dy_in, positions, w_q, w_k, w_v, w_o, w_pre, w_post, q_norm, k_norm):
        head = q_norm.shape[0]
        q_cols = w_q.shape[1] // n_dev
        kv_cols = w_k.shape[1] // n_dev
        heads = q_cols // head
        group = q_cols // kv_cols
        me = lax.axis_index('sp')
        batch = x_in.shape[0]
        wide = spans(NORM_CHUNKS)
        steps = spans(GRAD_CHUNKS)
        seqs = range(batch)
        home = [next((g, i - lo) for g, (lo, hi) in enumerate(wide) if lo <= i < hi) for i in seqs]
        turn = [next((g, i - lo) for g, (lo, hi) in enumerate(steps) if lo <= i < hi) for i in seqs]

        x_f32 = [x_in[i:i + 1].astype(jnp.float32) for i in seqs]
        normed = [gather(pre_norm_rows(x_in, w_pre, lo, hi)) for lo, hi in wide]
        cos_t, sin_t = rope_tables(lax.all_gather(positions, 'sp', axis=0, tiled=True), head)
        cos_t = cos_t.reshape(n_dev, -1, head)
        sin_t = sin_t.reshape(n_dev, -1, head)
        w_loc = jnp.concatenate([lax.dynamic_slice_in_dim(w_q, me * q_cols, q_cols, 1),
                                 lax.dynamic_slice_in_dim(w_k, me * kv_cols, kv_cols, 1),
                                 lax.dynamic_slice_in_dim(w_v, me * kv_cols, kv_cols, 1)], axis=1)
        wo_loc = lax.dynamic_slice_in_dim(w_o, me * q_cols, q_cols, 0)
        wq_row = q_norm[None, :]
        wk_row = k_norm[None, :]

        o_tok, qkv, o_loc, lse, y_parts, d_parts, d_proj_all = [], [], [], [], [], [], []
        dw_post = 0.0
        for i in seqs:
            g, first = home[i]
            if not first:
                qkv.append(ein('jbsd,dn->jbsn', normed[g], w_loc).astype(jnp.bfloat16))
            o_i, lse_i = attention_fwd(qkv[g], first, cos_t, sin_t, wq_row, wk_row, heads, group)
            o_loc.append(o_i)
            lse.append(lse_i)
            o_tok.append(swap(o_i))
            proj = ein('bsn,nd->bsd', join(o_tok[i]), w_o).astype(jnp.bfloat16)
            if i:
                proj, _ = lax.optimization_barrier((proj, d_parts[-1]))
            post, post_pull = jax.vjp(post_norm, proj, w_post)
            d_i, dwp = post_pull(dy_in[i:i + 1].astype(jnp.float32))
            dw_post = dw_post + dwp
            d_parts.append(d_i)
            y_parts.append((x_f32[i] + post).astype(jnp.bfloat16))
            step, _ = turn[i]
            lo, hi = steps[step]
            own = d_parts[lo:] if hi - lo == 1 else [jnp.concatenate(d_parts[lo:], axis=0)]
            if i + 1 == hi:
                d_proj_all.append(gather(own[0]))

        d_o = []
        dw_o = 0.0
        for step, (lo, hi) in enumerate(steps):
            for k in range(lo, hi):
                d_k = d_proj_all[step] if hi - lo == 1 else d_proj_all[step][:, k - lo:k - lo + 1]
                dw_o = dw_o + ein('jbsn,jbsd->nd', o_loc[k], d_k)
            dw_o = dw_o.astype(jnp.bfloat16) if hi == batch else lax.optimization_barrier(dw_o)
            d_o.append(ein('jbsd,nd->jbsn', d_proj_all[step], wo_loc).astype(jnp.bfloat16))

        d_tok, d_head = [], []
        dq_norm = 0.0
        dk_norm = 0.0
        for i in seqs:
            g, first = home[i]
            step, place = turn[i]
            deps = (d_head[i - 1],) if i else (d_parts[-1],)
            if i == AFTER_DWO:
                deps += (dw_o,)
            d_qkv, dwq, dwk = attention_bwd(qkv[g], first, d_o[step], place, lse[i], cos_t, sin_t, wq_row, wk_row, heads, group, deps)
            dq_norm = dq_norm + jnp.sum(dwq, axis=0)
            dk_norm = dk_norm + jnp.sum(dwk, axis=0)
            d_head.append(d_qkv)
            d_tok.append(swap(d_qkv))

        def gather_to(axis):
            return lambda arr: lax.all_gather(arr, 'sp', axis=axis, tiled=True)

        dw_o = settle(gather_to(0)(dw_o), 8)
        qk = q_cols + kv_cols
        dw_qk, dw_v = 0.0, 0.0
        for g in range(len(wide)):
            own = [d_head[i] for i in seqs if home[i][0] == g]
            for i, d in enumerate(own):
                n_g = normed[g] if len(own) == 1 else normed[g][:, i:i + 1]
                dw_qk = dw_qk + ein('jbsd,jbsn->dn', n_g, d[..., :qk])
            for i, d in enumerate(own):
                n_g = normed[g] if len(own) == 1 else normed[g][:, i:i + 1]
                dw_v = dw_v + ein('jbsd,jbsn->dn', n_g, d[..., qk:])
            if g == 0:
                dw_qk = lax.optimization_barrier(dw_qk)
                dw_v = lax.optimization_barrier(dw_v)
        dw_q, dw_k = split_qk(gather_to(1)(dw_qk.astype(jnp.bfloat16)), n_dev, w_q.shape[1], w_k.shape[1], 9)
        dw_v = settle(gather_to(1)(dw_v.astype(jnp.bfloat16)), 6)

        dx_parts = []
        dw_pre = 0.0
        for lo, hi in wide:
            tok = jnp.concatenate(d_tok[lo:hi], axis=1)
            dq = join(tok[..., :q_cols])
            dk = join(tok[..., q_cols:qk])
            dv = join(tok[..., qk:])
            d_normed = (ein('bsn,dn->bsd', dq, w_q) + ein('bsn,dn->bsd', dk, w_k) + ein('bsn,dn->bsd', dv, w_v)).astype(jnp.bfloat16)
            dx_norm, dwp = jax.vjp(pre_norm, x_in[lo:hi].astype(jnp.float32), w_pre)[1](d_normed)
            dw_pre = dw_pre + dwp
            dx_parts.append((dy_in[lo:hi].astype(jnp.float32) + dx_norm).astype(jnp.bfloat16))

        sums = lax.psum((dw_pre, dw_post, dq_norm, dk_norm), 'sp')
        return (jnp.concatenate(y_parts, axis=0), jnp.concatenate(dx_parts, axis=0), dw_q, dw_k, dw_v, dw_o) + sums

    token_spec = P('dp', 'sp', None)
    return jax.shard_map(layer, mesh=mesh,
                         in_specs=(token_spec, token_spec, P(('dp', 'sp')), P(None, None), P(None, None), P(None, None), P(None, None), P(None), P(None), P(None), P(None)),
                         out_specs=(token_spec, token_spec, P('dp', None), P('dp', None), P('dp', None), P('dp', None), P('dp'), P('dp'), P('dp'), P('dp')),
                         check_vma=False)
```
